32 devices in a mesh: frame: 4 (over y, core), row: 8 (over z, x).
Axes of the slice: x: 2, y: 2, z: 4, core: 2. Of those that a mesh axis runs over, the one named last changes fastest.
Arguments:
- features: float32 [4, 32, 256, 256], P('frame', 'row'), may hold values from -6 to 6
- conv_weight: float32 [2, 3, 3, 256, 256], replicated, may hold values from -0.125 to 0.125
Outputs:
- activations: float32 [4, 32, 256, 256], P('frame', 'row')
The draws below stay inside these ranges and needn't reach their ends.
All inputs are finite; a program needn't handle non-finite values.
Results may differ from the reference program's by a relative error of at most 0.0001.
Values sent between devices are 32-bit elements; how exact they have to be, the bound alone decides.
A program may use at most 64 MiB of HBM per device.

```python
import jax
import jax.numpy as jnp
from jax import lax

C = 256
W = 256
LAYERS = 2
FRAMES = 4
H = 32


def block_levels(key, shape, shards, least, top_value):
    def one(position, shards_of):
        steps = jax.random.uniform(jax.random.fold_in(jax.random.fold_in(key, 6), position), (shards_of,), jnp.float32, least / len(shards), top_value / len(shards))
        return jnp.repeat(jnp.exp(steps), shape[position] // shards_of).reshape((-1,) + (1,) * (len(shape) - position - 1))

    factor_of = one(*shards[0])
    for cut in shards[1:]:
        factor_of = factor_of * one(*cut)
    return factor_of


def scatter_about(key, dims, deviation, reach, pieces=(), kind=jnp.bfloat16):
    factor_of = block_levels(key, dims, pieces, -0.22, 0.18) if pieces else 1.0
    result = jax.random.normal(key, dims, jnp.float32) * deviation * factor_of
    return jnp.minimum(jnp.maximum(result, -reach), reach).astype(kind)


def setup_inputs(seed: int = 0) -> dict:
    keys = jax.random.split(jax.random.key(seed), 3)
    features = scatter_about(keys[0], (FRAMES, H, W, C), 1.0, 6.0, ((0, 4), (1, 8)), jnp.float32)
    conv_weight = scatter_about(keys[1], (LAYERS, 3, 3, C, C), (9 * C) ** -0.5, 0.125, (), jnp.float32)
    return dict(features=features, conv_weight=conv_weight)


def temporal_shift(field):
    fold = field.shape[3] // 8
    zeros = jnp.zeros_like(field[:1, :, :, :fold])
    from_next = jnp.concatenate([field[1:, :, :, :fold], zeros], axis=0)
    from_prev = jnp.concatenate([zeros, field[:-1, :, :, fold:2 * fold]], axis=0)
    return jnp.concatenate([from_next, from_prev, field[:, :, :, 2 * fold:]], axis=3)


def convolve_frame(frame, kernel):
    rows, cols, chans = frame.shape
    padded = jnp.pad(frame, ((1, 1), (1, 1), (0, 0)))
    total = jnp.zeros((rows * cols, kernel.shape[3]), jnp.float32)
    for tap_row in range(3):
        for tap_col in range(3):
            window = padded[tap_row:tap_row + rows, tap_col:tap_col + cols, :].reshape(rows * cols, chans)
            total = total + jnp.dot(window, kernel[tap_row, tap_col], preferred_element_type=jnp.float32, precision=lax.Precision.HIGHEST)
    return jnp.maximum(total, 0.0).reshape(rows, cols, kernel.shape[3])


def reference(features, conv_weight):
    field = features
    for layer in range(LAYERS):
        shifted = temporal_shift(field)
        kernel = conv_weight[layer]
        field = lax.map(lambda frame: convolve_frame(frame, kernel), shifted)
    return field
```

```python
import functools

import jax
import jax.numpy as jnp
from jax import lax
from jax.experimental import pallas as pl
from jax.experimental.pallas import tpu as pltpu
from jax.sharding import PartitionSpec as P

MESH = pl.DeviceIdType.MESH
LANES = 128
PAD = 8


def split(value):
    high = value.astype(jnp.bfloat16)
    low = (value - high.astype(jnp.float32)).astype(jnp.bfloat16)
    return high, low


def kernel(
    cuts, x_hbm, w_hbm, o_hbm, xin, wbuf, w3, sx, acc, mid, halo, edge, pack, got, out,
    load_sem, store_sem, row_send, row_recv, frame_send, frame_recv,
):
    rows, cols, chans = xin.shape
    layers = wbuf.shape[0]
    fold = chans // 8
    last = rows - 1
    frames, bands = lax.axis_size("frame"), lax.axis_size("row")
    t, r = lax.axis_index("frame"), lax.axis_index("row")
    has_row = (r > 0, r < bands - 1)
    has_frame = (t > 0, t < frames - 1)
    row_to = (r - 1, r + 1)
    frame_to = (t - 1, t + 1)

    load_x = pltpu.make_async_copy(x_hbm.at[0], xin, load_sem.at[layers])
    load_x.start()
    load_w = [pltpu.make_async_copy(w_hbm.at[n], wbuf.at[n], load_sem.at[n]) for n in range(layers)]
    for load in load_w:
        load.start()

    barrier = pltpu.get_barrier_semaphore()
    count = 0
    for have, axis, peers in ((has_row, "row", row_to), (has_frame, "frame", frame_to)):
        for side in range(2):
            count = count + have[side].astype(jnp.int32)

            @pl.when(have[side])
            def _():
                pl.semaphore_signal(barrier, inc=1, device_id={axis: peers[side]}, device_id_type=MESH)

    pl.semaphore_wait(barrier, count)

    def maps(layer):
        return xin if layer == 0 else mid.at[layer - 1]

    def span(layer, chunk):
        return cuts[layer][chunk], cuts[layer][chunk + 1] - cuts[layer][chunk]

    def row_copy(layer, side, tile, chunk):
        start, size = span(layer, chunk)
        row = 0 if side == 0 else last
        if tile == 1:
            source = maps(layer).at[row, pl.ds(start, size), pl.ds(LANES, LANES)]
        else:
            source = edge.at[layer, side, pl.ds(start, size)]
        return pltpu.make_async_remote_copy(
            src_ref=source,
            dst_ref=halo.at[layer, 1 - side, tile, pl.ds(start, size)],
            send_sem=row_send.at[layer, side, tile, chunk],
            recv_sem=row_recv.at[layer, side, tile, chunk],
            device_id={"row": row_to[side]},
            device_id_type=MESH,
        )

    def frame_copy(layer, side, chunk):
        start, size = span(layer, chunk)
        return pltpu.make_async_remote_copy(
            src_ref=pack.at[layer, side, pl.ds(start, size)],
            dst_ref=got.at[layer, side, pl.ds(start, size)],
            send_sem=frame_send.at[layer, side, chunk],
            recv_sem=frame_recv.at[layer, side, chunk],
            device_id={"frame": frame_to[side]},
            device_id_type=MESH,
        )

    def send_rows(layer, tile, chunk):
        for side in range(2):

            @pl.when(has_row[side])
            def _():
                row_copy(layer, side, tile, chunk).start()

    def send_frames(layer, chunk):
        start, size = span(layer, chunk)
        lane = lax.broadcasted_iota(jnp.int32, (size, LANES), 1)
        for side in range(2):
            full = jnp.zeros((size, LANES), jnp.float32)
            for row in range(rows):
                value = maps(layer)[row, pl.ds(start, size), pl.ds(0, LANES)]
                shift = ((row - side) * fold) % LANES
                value = pltpu.roll(value, shift, 1) if shift else value
                full = jnp.where(lane // fold == row, value, full)
            pack[layer, side, pl.ds(start, size)] = full

            @pl.when(has_frame[side])
            def _():
                frame_copy(layer, side, chunk).start()

    def take_frames(layer, chunk):
        start, size = span(layer, chunk)
        for side in range(2):

            @pl.when(has_frame[1 - side])
            def _():
                frame_copy(layer, side, chunk).wait_recv()

            @pl.when(jnp.logical_not(has_frame[1 - side]))
            def _():
                got[layer, side, pl.ds(start, size)] = jnp.zeros((size, LANES), jnp.float32)

    def shifted_tile(layer, chunk, row):
        start, size = span(layer, chunk)
        lane = lax.broadcasted_iota(jnp.int32, (size, LANES), 1)
        value = maps(layer)[row, pl.ds(start, size), pl.ds(0, LANES)]
        for side in range(2):
            part = got[layer, side, pl.ds(start, size)]
            shift = ((side - row) * fold) % LANES
            part = pltpu.roll(part, shift, 1) if shift else part
            value = jnp.where(lane // fold == side, part, value)
        return value

    def put(row, start, size, tile, value):
        high, low = split(value)
        sx[row, pl.ds(start, size), pl.ds(tile * LANES, LANES)] = high
        sx[row, pl.ds(start, size), pl.ds(chans + tile * LANES, LANES)] = low
        sx[row, pl.ds(start, size), pl.ds(2 * chans + tile * LANES, LANES)] = high

    def lower_edges(layer, chunk):
        start, size = span(layer, chunk)
        for row in range(rows):
            value = shifted_tile(layer, chunk, row)
            if row == 0:
                edge[layer, 0, pl.ds(start, size)] = value
            if row == last:
                edge[layer, 1, pl.ds(start, size)] = value
        send_rows(layer, 0, chunk)

    def fill(layer):
        for chunk in range(len(cuts[layer]) - 1):
            start, size = span(layer, chunk)
            for row in range(rows):
                put(row + 1, start, size, 0, shifted_tile(layer, chunk, row))
                put(row + 1, start, size, 1, maps(layer)[row, pl.ds(start, size), pl.ds(LANES, LANES)])
        blank = jnp.zeros((cols, 3 * chans), jnp.bfloat16)
        sx[0] = blank
        sx[rows + 1] = blank

    def split_weights(layer):
        load_w[layer].wait()

        def tap(index, carry):
            down, across = index // 3, index % 3
            high, low = split(wbuf[layer, down, across])
            base = pl.multiple_of(down * 3 * chans, 3 * chans)
            w3[layer, across, pl.ds(base, chans)] = high
            w3[layer, across, pl.ds(base + chans, chans)] = high
            w3[layer, across, pl.ds(base + 2 * chans, chans)] = low
            return carry

        lax.fori_loop(0, 9, tap, 0)

    def inner(layer):
        def across(tap, carry):
            left = jnp.concatenate(
                [sx[pl.ds(down, rows)].reshape(rows * cols, 3 * chans) for down in range(3)], axis=1
            )
            total = jnp.dot(left, w3[layer, tap], preferred_element_type=jnp.float32)
            acc[tap, :, pl.ds(PAD, cols)] = total.reshape(rows, cols, chans)
            return carry

        lax.fori_loop(0, 3, across, 0)

    def finish(row, start, size):
        total = acc[0, row, pl.ds(PAD + start - 1, size)] + acc[1, row, pl.ds(PAD + start, size)]
        total = total + acc[2, row, pl.ds(PAD + start + 1, size)]
        return jnp.maximum(total, 0.0)

    def outer(layer, chunk):
        start, size = span(layer, chunk)
        for side in range(2):
            place = 0 if side == 0 else rows + 1

            @pl.when(has_row[side])
            def _():
                for tile in range(2):
                    row_copy(layer, 1 - side, tile, chunk).wait_recv()
                for tile in range(2):
                    put(place, start, size, tile, halo[layer, side, tile, pl.ds(start, size)])

        def across(tap, carry):
            for place, row, down in ((0, 0, 0), (rows + 1, last, 2)):
                extra = jnp.dot(
                    sx[place, pl.ds(start, size)],
                    w3[layer, tap, pl.ds(down * 3 * chans, 3 * chans)],
                    preferred_element_type=jnp.float32,
                )
                acc[tap, row, pl.ds(PAD + start, size)] += extra
            return carry

        lax.fori_loop(0, 3, across, 0)

    chunks = len(cuts[0]) - 1
    load_x.wait()
    for chunk in range(chunks):
        send_rows(0, 1, chunk)
    for chunk in range(chunks):
        send_frames(0, chunk)
    acc[:, :, pl.ds(0, PAD)] = jnp.zeros((3, rows, PAD, chans), jnp.float32)
    acc[:, :, pl.ds(PAD + cols, PAD)] = jnp.zeros((3, rows, PAD, chans), jnp.float32)
    for chunk in range(chunks):
        take_frames(0, chunk)
        lower_edges(0, chunk)
    split_weights(0)
    for layer in range(layers):
        final = layer == layers - 1
        fill(layer)
        inner(layer)
        if not final:
            split_weights(layer + 1)
        target = out if final else mid.at[layer]
        for row in range(1, last):
            target[row] = finish(row, 0, cols)
            if final:
                pltpu.make_async_copy(out.at[row], o_hbm.at[0, row], store_sem.at[row]).start()
        for chunk in range(chunks):
            outer(layer, chunk)
            start = cuts[layer + 1][chunk]
            size = cuts[layer + 1][chunk + 1] - start
            for row in (0, last):
                target[row, pl.ds(start, size)] = finish(row, start, size)
            if not final:
                send_rows(layer + 1, 1, chunk)
                send_frames(layer + 1, chunk)
                take_frames(layer + 1, chunk)
                lower_edges(layer + 1, chunk)
        if final:
            for row in (0, last):
                pltpu.make_async_copy(out.at[row], o_hbm.at[0, row], store_sem.at[row]).start()

    for layer in range(layers):
        for chunk in range(chunks):
            for side in range(2):

                @pl.when(has_row[side])
                def _():
                    for tile in range(2):
                        row_copy(layer, side, tile, chunk).wait_send()

                @pl.when(has_frame[side])
                def _():
                    frame_copy(layer, side, chunk).wait_send()

    for row in range(rows):
        pltpu.make_async_copy(out.at[row], o_hbm.at[0, row], store_sem.at[row]).wait()


def local(features, conv_weight):
    _, rows, cols, chans = features.shape
    layers = conv_weight.shape[0]
    half, step = cols // 2, 2 * PAD
    cuts = [[0, half + step * (layers - 1 - n), cols] for n in range(layers)] + [[0, half - step, cols]]
    chunks = len(cuts[0]) - 1
    f32, bf16 = jnp.float32, jnp.bfloat16
    dma = pltpu.SemaphoreType.DMA
    return pl.pallas_call(
        functools.partial(kernel, cuts),
        out_shape=jax.ShapeDtypeStruct(features.shape, f32),
        in_specs=[pl.BlockSpec(memory_space=pl.ANY)] * 2,
        out_specs=pl.BlockSpec(memory_space=pl.ANY),
        scratch_shapes=[
            pltpu.VMEM((rows, cols, chans), f32),
            pltpu.VMEM(conv_weight.shape, f32),
            pltpu.VMEM((layers, 3, 9 * chans, chans), bf16),
            pltpu.VMEM((rows + 2, cols, 3 * chans), bf16),
            pltpu.VMEM((3, rows, cols + 2 * PAD, chans), f32),
            pltpu.VMEM((layers - 1, rows, cols, chans), f32),
            pltpu.VMEM((layers, 2, 2, cols, LANES), f32),
            pltpu.VMEM((layers, 2, cols, LANES), f32),
            pltpu.VMEM((layers, 2, cols, LANES), f32),
            pltpu.VMEM((layers, 2, cols, LANES), f32),
            pltpu.VMEM((rows, cols, chans), f32),
            dma((layers + 1,)),
            dma((rows,)),
            dma((layers, 2, 2, chunks)),
            dma((layers, 2, 2, chunks)),
            dma((layers, 2, chunks)),
            dma((layers, 2, chunks)),
        ],
        compiler_params=pltpu.CompilerParams(
            collective_id=0, has_side_effects=True, vmem_limit_bytes=60 * 1024 * 1024
        ),
    )(features, conv_weight)


def solution(mesh):
    placed = (P("frame", "row", None, None), P())
    return jax.shard_map(
        local, mesh=mesh, in_specs=placed, out_specs=P("frame", "row", None, None), check_vma=False
    )
```

```python
import functools

import jax
import jax.numpy as jnp
from jax import lax
from jax.experimental import pallas as pl
from jax.experimental.pallas import tpu as pltpu
from jax.sharding import PartitionSpec as P

MESH = pl.DeviceIdType.MESH
LANES = 128
PAD = 8


def split(value):
    high = value.astype(jnp.bfloat16)
    low = (value - high.astype(jnp.float32)).astype(jnp.bfloat16)
    return high, low


def kernel(
    cuts, x_hbm, w_hbm, out, xin, wbuf, w3, sx, acc, mid, halo, edge, pack, got,
    load_sem, row_send, row_recv, frame_send, frame_recv,
):
    rows, cols, chans = xin.shape
    layers = wbuf.shape[0]
    fold = chans // 8
    last = rows - 1
    frames, bands = lax.axis_size("frame"), lax.axis_size("row")
    t, r = lax.axis_index("frame"), lax.axis_index("row")
    has_row = (r > 0, r < bands - 1)
    has_frame = (t > 0, t < frames - 1)
    row_to = (r - 1, r + 1)
    frame_to = (t - 1, t + 1)

    load_x = pltpu.make_async_copy(x_hbm.at[0], xin, load_sem.at[layers])
    load_x.start()
    load_w = [pltpu.make_async_copy(w_hbm.at[n], wbuf.at[n], load_sem.at[n]) for n in range(layers)]
    for load in load_w:
        load.start()

    barrier = pltpu.get_barrier_semaphore()
    count = 0
    for have, axis, peers in ((has_row, "row", row_to), (has_frame, "frame", frame_to)):
        for side in range(2):
            count = count + have[side].astype(jnp.int32)

            @pl.when(have[side])
            def _():
                pl.semaphore_signal(barrier, inc=1, device_id={axis: peers[side]}, device_id_type=MESH)

    pl.semaphore_wait(barrier, count)

    def maps(layer):
        return xin if layer == 0 else mid.at[layer - 1]

    def span(layer, chunk):
        return cuts[layer][chunk], cuts[layer][chunk + 1] - cuts[layer][chunk]

    def row_copy(layer, side, tile, chunk):
        start, size = span(layer, chunk)
        row = 0 if side == 0 else last
        if tile == 1:
            source = maps(layer).at[row, pl.ds(start, size), pl.ds(LANES, LANES)]
        else:
            source = edge.at[layer, side, pl.ds(start, size)]
        return pltpu.make_async_remote_copy(
            src_ref=source,
            dst_ref=halo.at[layer, 1 - side, tile, pl.ds(start, size)],
            send_sem=row_send.at[layer, side, tile, chunk],
            recv_sem=row_recv.at[layer, side, tile, chunk],
            device_id={"row": row_to[side]},
            device_id_type=MESH,
        )

    def frame_copy(layer, side, chunk):
        start, size = span(layer, chunk)
        return pltpu.make_async_remote_copy(
            src_ref=pack.at[layer, side, pl.ds(start, size)],
            dst_ref=got.at[layer, side, pl.ds(start, size)],
            send_sem=frame_send.at[layer, side, chunk],
            recv_sem=frame_recv.at[layer, side, chunk],
            device_id={"frame": frame_to[side]},
            device_id_type=MESH,
        )

    def send_rows(layer, tile, chunk):
        for side in range(2):

            @pl.when(has_row[side])
            def _():
                row_copy(layer, side, tile, chunk).start()

    def send_frames(layer, chunk):
        start, size = span(layer, chunk)
        lane = lax.broadcasted_iota(jnp.int32, (size, LANES), 1)
        for side in range(2):
            full = jnp.zeros((size, LANES), jnp.float32)
            for row in range(rows):
                value = maps(layer)[row, pl.ds(start, size), pl.ds(0, LANES)]
                shift = ((row - side) * fold) % LANES
                value = pltpu.roll(value, shift, 1) if shift else value
                full = jnp.where(lane // fold == row, value, full)
            pack[layer, side, pl.ds(start, size)] = full

            @pl.when(has_frame[side])
            def _():
                frame_copy(layer, side, chunk).start()

    def take_frames(layer, chunk):
        start, size = span(layer, chunk)
        for side in range(2):

            @pl.when(has_frame[1 - side])
            def _():
                frame_copy(layer, side, chunk).wait_recv()

            @pl.when(jnp.logical_not(has_frame[1 - side]))
            def _():
                got[layer, side, pl.ds(start, size)] = jnp.zeros((size, LANES), jnp.float32)

    def shifted_tile(layer, chunk, row):
        start, size = span(layer, chunk)
        lane = lax.broadcasted_iota(jnp.int32, (size, LANES), 1)
        value = maps(layer)[row, pl.ds(start, size), pl.ds(0, LANES)]
        for side in range(2):
            part = got[layer, side, pl.ds(start, size)]
            shift = ((side - row) * fold) % LANES
            part = pltpu.roll(part, shift, 1) if shift else part
            value = jnp.where(lane // fold == side, part, value)
        return value

    def put(row, start, size, tile, value):
        high, low = split(value)
        sx[row, pl.ds(start, size), pl.ds(tile * LANES, LANES)] = high
        sx[row, pl.ds(start, size), pl.ds(chans + tile * LANES, LANES)] = low
        sx[row, pl.ds(start, size), pl.ds(2 * chans + tile * LANES, LANES)] = high

    def lower_edges(layer, chunk):
        start, size = span(layer, chunk)
        for row in range(rows):
            value = shifted_tile(layer, chunk, row)
            if row == 0:
                edge[layer, 0, pl.ds(start, size)] = value
            if row == last:
                edge[layer, 1, pl.ds(start, size)] = value
        send_rows(layer, 0, chunk)

    def fill(layer):
        for chunk in range(len(cuts[layer]) - 1):
            start, size = span(layer, chunk)
            for row in range(rows):
                put(row + 1, start, size, 0, shifted_tile(layer, chunk, row))
                put(row + 1, start, size, 1, maps(layer)[row, pl.ds(start, size), pl.ds(LANES, LANES)])
        blank = jnp.zeros((cols, 3 * chans), jnp.bfloat16)
        sx[0] = blank
        sx[rows + 1] = blank

    def split_weights(layer):
        load_w[layer].wait()

        def tap(index, carry):
            down, across = index // 3, index % 3
            high, low = split(wbuf[layer, down, across])
            base = pl.multiple_of(down * 3 * chans, 3 * chans)
            w3[layer, across, pl.ds(base, chans)] = high
            w3[layer, across, pl.ds(base + chans, chans)] = high
            w3[layer, across, pl.ds(base + 2 * chans, chans)] = low
            return carry

        lax.fori_loop(0, 9, tap, 0)

    def inner(layer):
        def across(tap, carry):
            left = jnp.concatenate(
                [sx[pl.ds(down, rows)].reshape(rows * cols, 3 * chans) for down in range(3)], axis=1
            )
            total = jnp.dot(left, w3[layer, tap], preferred_element_type=jnp.float32)
            acc[tap, :, pl.ds(PAD, cols)] = total.reshape(rows, cols, chans)
            return carry

        lax.fori_loop(0, 3, across, 0)

    def finish(row, start, size):
        total = acc[0, row, pl.ds(PAD + start - 1, size)] + acc[1, row, pl.ds(PAD + start, size)]
        total = total + acc[2, row, pl.ds(PAD + start + 1, size)]
        return jnp.maximum(total, 0.0)

    def outer(layer, chunk):
        start, size = span(layer, chunk)
        for side in range(2):
            place = 0 if side == 0 else rows + 1

            @pl.when(has_row[side])
            def _():
                for tile in range(2):
                    row_copy(layer, 1 - side, tile, chunk).wait_recv()
                for tile in range(2):
                    put(place, start, size, tile, halo[layer, side, tile, pl.ds(start, size)])

        def across(tap, carry):
            for place, row, down in ((0, 0, 0), (rows + 1, last, 2)):
                extra = jnp.dot(
                    sx[place, pl.ds(start, size)],
                    w3[layer, tap, pl.ds(down * 3 * chans, 3 * chans)],
                    preferred_element_type=jnp.float32,
                )
                acc[tap, row, pl.ds(PAD + start, size)] += extra
            return carry

        lax.fori_loop(0, 3, across, 0)

    chunks = len(cuts[0]) - 1
    load_x.wait()
    for chunk in range(chunks):
        send_rows(0, 1, chunk)
    for chunk in range(chunks):
        send_frames(0, chunk)
    acc[:, :, pl.ds(0, PAD)] = jnp.zeros((3, rows, PAD, chans), jnp.float32)
    acc[:, :, pl.ds(PAD + cols, PAD)] = jnp.zeros((3, rows, PAD, chans), jnp.float32)
    for chunk in range(chunks):
        take_frames(0, chunk)
        lower_edges(0, chunk)
    split_weights(0)
    for layer in range(layers):
        final = layer == layers - 1
        fill(layer)
        inner(layer)
        if not final:
            split_weights(layer + 1)
        target = out if final else mid.at[layer]
        for row in range(1, last):
            target[row] = finish(row, 0, cols)
        for chunk in range(chunks):
            outer(layer, chunk)
            start = cuts[layer + 1][chunk]
            size = cuts[layer + 1][chunk + 1] - start
            for row in (0, last):
                target[row, pl.ds(start, size)] = finish(row, start, size)
            if not final:
                send_rows(layer + 1, 1, chunk)
                send_frames(layer + 1, chunk)
                take_frames(layer + 1, chunk)
                lower_edges(layer + 1, chunk)

    for layer in range(layers):
        for chunk in range(chunks):
            for side in range(2):

                @pl.when(has_row[side])
                def _():
                    for tile in range(2):
                        row_copy(layer, side, tile, chunk).wait_send()

                @pl.when(has_frame[side])
                def _():
                    frame_copy(layer, side, chunk).wait_send()


def store(y_ref, o_hbm, sem):
    copies = [pltpu.make_async_copy(y_ref.at[n], o_hbm.at[0, n], sem.at[n]) for n in range(y_ref.shape[0])]
    for copy in copies:
        copy.start()
    for copy in copies:
        copy.wait()


def local(features, conv_weight):
    _, rows, cols, chans = features.shape
    layers = conv_weight.shape[0]
    half, step = cols // 2, 2 * PAD
    cuts = [[0, half + step * (layers - 1 - n), cols] for n in range(layers)] + [[0, half - step, cols]]
    chunks = len(cuts[0]) - 1
    f32, bf16 = jnp.float32, jnp.bfloat16
    dma = pltpu.SemaphoreType.DMA
    result = pl.pallas_call(
        functools.partial(kernel, cuts),
        out_shape=pltpu.VMEM((rows, cols, chans), f32),
        in_specs=[pl.BlockSpec(memory_space=pl.ANY)] * 2,
        out_specs=pl.BlockSpec(memory_space=pltpu.VMEM),
        scratch_shapes=[
            pltpu.VMEM((rows, cols, chans), f32),
            pltpu.VMEM(conv_weight.shape, f32),
            pltpu.VMEM((layers, 3, 9 * chans, chans), bf16),
            pltpu.VMEM((rows + 2, cols, 3 * chans), bf16),
            pltpu.VMEM((3, rows, cols + 2 * PAD, chans), f32),
            pltpu.VMEM((layers - 1, rows, cols, chans), f32),
            pltpu.VMEM((layers, 2, 2, cols, LANES), f32),
            pltpu.VMEM((layers, 2, cols, LANES), f32),
            pltpu.VMEM((layers, 2, cols, LANES), f32),
            pltpu.VMEM((layers, 2, cols, LANES), f32),
            dma((layers + 1,)),
            dma((layers, 2, 2, chunks)),
            dma((layers, 2, 2, chunks)),
            dma((layers, 2, chunks)),
            dma((layers, 2, chunks)),
        ],
        compiler_params=pltpu.CompilerParams(
            collective_id=0, has_side_effects=True, vmem_limit_bytes=62 * 1024 * 1024
        ),
    )(features, conv_weight)
    return pl.pallas_call(
        store,
        out_shape=jax.ShapeDtypeStruct(features.shape, f32),
        in_specs=[pl.BlockSpec(memory_space=pltpu.VMEM)],
        out_specs=pl.BlockSpec(memory_space=pl.ANY),
        scratch_shapes=[dma((rows,))],
        compiler_params=pltpu.CompilerParams(vmem_limit_bytes=2 * 1024 * 1024),
    )(result)


def solution(mesh):
    placed = (P("frame", "row", None, None), P())
    return jax.shard_map(
        local, mesh=mesh, in_specs=placed, out_specs=P("frame", "row", None, None), check_vma=False
    )
```

```python
import functools

import jax
import jax.numpy as jnp
from jax import lax
from jax.experimental import pallas as pl
from jax.experimental.pallas import tpu as pltpu
from jax.sharding import PartitionSpec as P

MESH = pl.DeviceIdType.MESH
LANES = 128
PAD = 8


def split(value):
    high = value.astype(jnp.bfloat16)
    low = (value - high.astype(jnp.float32)).astype(jnp.bfloat16)
    return high, low


def kernel(
    cuts, x_hbm, w_hbm, out, xin, wbuf, w3, sx, acc, mid, halo, edge, pack, got,
    load_sem, row_send, row_recv, frame_send, frame_recv,
):
    rows, cols, chans = xin.shape
    layers = wbuf.shape[0]
    fold = chans // 8
    last = rows - 1
    frames, bands = lax.axis_size("frame"), lax.axis_size("row")
    t, r = lax.axis_index("frame"), lax.axis_index("row")
    has_row = (r > 0, r < bands - 1)
    has_frame = (t > 0, t < frames - 1)
    row_to = (r - 1, r + 1)
    frame_to = (t - 1, t + 1)

    load_x = pltpu.make_async_copy(x_hbm.at[0], xin, load_sem.at[layers])
    load_x.start()
    load_w = [pltpu.make_async_copy(w_hbm.at[n], wbuf.at[n], load_sem.at[n]) for n in range(layers)]
    for load in load_w:
        load.start()

    barrier = pltpu.get_barrier_semaphore()
    count = 0
    for have, axis, peers in ((has_row, "row", row_to), (has_frame, "frame", frame_to)):
        for side in range(2):
            count = count + have[side].astype(jnp.int32)

            @pl.when(have[side])
            def _():
                pl.semaphore_signal(barrier, inc=1, device_id={axis: peers[side]}, device_id_type=MESH)

    pl.semaphore_wait(barrier, count)

    def maps(layer):
        return xin if layer == 0 else mid.at[layer - 1]

    def span(layer, chunk):
        return cuts[layer][chunk], cuts[layer][chunk + 1] - cuts[layer][chunk]

    def row_copy(layer, side, tile, chunk):
        start, size = span(layer, chunk)
        row = 0 if side == 0 else last
        if tile == 1:
            source = maps(layer).at[row, pl.ds(start, size), pl.ds(LANES, LANES)]
        else:
            source = edge.at[layer, side, pl.ds(start, size)]
        return pltpu.make_async_remote_copy(
            src_ref=source,
            dst_ref=halo.at[layer, 1 - side, tile, pl.ds(start, size)],
            send_sem=row_send.at[layer, side, tile, chunk],
            recv_sem=row_recv.at[layer, side, tile, chunk],
            device_id={"row": row_to[side]},
            device_id_type=MESH,
        )

    def frame_copy(layer, side, chunk):
        start, size = span(layer, chunk)
        return pltpu.make_async_remote_copy(
            src_ref=pack.at[layer, side, pl.ds(start, size)],
            dst_ref=got.at[layer, side, pl.ds(start, size)],
            send_sem=frame_send.at[layer, side, chunk],
            recv_sem=frame_recv.at[layer, side, chunk],
            device_id={"frame": frame_to[side]},
            device_id_type=MESH,
        )

    def send_rows(layer, tile, chunk):
        for side in range(2):

            @pl.when(has_row[side])
            def _():
                row_copy(layer, side, tile, chunk).start()

    def send_frames(layer, chunk):
        start, size = span(layer, chunk)
        lane = lax.broadcasted_iota(jnp.int32, (size, LANES), 1)
        for side in range(2):
            full = jnp.zeros((size, LANES), jnp.float32)
            for row in range(rows):
                value = maps(layer)[row, pl.ds(start, size), pl.ds(0, LANES)]
                shift = ((row - side) * fold) % LANES
                value = pltpu.roll(value, shift, 1) if shift else value
                full = jnp.where(lane // fold == row, value, full)
            pack[layer, side, pl.ds(start, size)] = full

            @pl.when(has_frame[side])
            def _():
                frame_copy(layer, side, chunk).start()

    def take_frames(layer, chunk):
        start, size = span(layer, chunk)
        for side in range(2):

            @pl.when(has_frame[1 - side])
            def _():
                frame_copy(layer, side, chunk).wait_recv()

            @pl.when(jnp.logical_not(has_frame[1 - side]))
            def _():
                got[layer, side, pl.ds(start, size)] = jnp.zeros((size, LANES), jnp.float32)

    def shifted_tile(layer, chunk, row):
        start, size = span(layer, chunk)
        lane = lax.broadcasted_iota(jnp.int32, (size, LANES), 1)
        value = maps(layer)[row, pl.ds(start, size), pl.ds(0, LANES)]
        for side in range(2):
            part = got[layer, side, pl.ds(start, size)]
            shift = ((side - row) * fold) % LANES
            part = pltpu.roll(part, shift, 1) if shift else part
            value = jnp.where(lane // fold == side, part, value)
        return value

    def put(row, start, size, tile, value):
        high, low = split(value)
        sx[row, pl.ds(start, size), pl.ds(tile * LANES, LANES)] = high
        sx[row, pl.ds(start, size), pl.ds(chans + tile * LANES, LANES)] = low
        sx[row, pl.ds(start, size), pl.ds(2 * chans + tile * LANES, LANES)] = high

    def lower_edges(layer, chunk):
        start, size = span(layer, chunk)
        for row in range(rows):
            value = shifted_tile(layer, chunk, row)
            if row == 0:
                edge[layer, 0, pl.ds(start, size)] = value
            if row == last:
                edge[layer, 1, pl.ds(start, size)] = value
        send_rows(layer, 0, chunk)

    def fill(layer):
        for chunk in range(len(cuts[layer]) - 1):
            start, size = span(layer, chunk)
            for row in range(rows):
                put(row + 1, start, size, 0, shifted_tile(layer, chunk, row))
                put(row + 1, start, size, 1, maps(layer)[row, pl.ds(start, size), pl.ds(LANES, LANES)])
        blank = jnp.zeros((cols, 3 * chans), jnp.bfloat16)
        sx[0] = blank
        sx[rows + 1] = blank

    def split_weights(layer):
        load_w[layer].wait()

        def tap(index, carry):
            down, across = index // 3, index % 3
            high, low = split(wbuf[layer, down, across])
            base = pl.multiple_of(down * 3 * chans, 3 * chans)
            w3[layer, across, pl.ds(base, chans)] = high
            w3[layer, across, pl.ds(base + chans, chans)] = high
            w3[layer, across, pl.ds(base + 2 * chans, chans)] = low
            return carry

        lax.fori_loop(0, 9, tap, 0)

    def inner(layer):
        def across(tap, carry):
            for first, count, low, high in ((0, 1, 1, 3), (1, rows - 2, 0, 3), (last, 1, 0, 2)):
                left = jnp.concatenate(
                    [
                        sx[pl.ds(first + down, count)].reshape(count * cols, 3 * chans)
                        for down in range(low, high)
                    ],
                    axis=1,
                )
                taps = w3[layer, tap, pl.ds(low * 3 * chans, (high - low) * 3 * chans)]
                total = jnp.dot(left, taps, preferred_element_type=jnp.float32)
                acc[tap, pl.ds(first, count), pl.ds(PAD, cols)] = total.reshape(count, cols, chans)
            return carry

        lax.fori_loop(0, 3, across, 0)

    def finish(row, start, size):
        total = acc[0, row, pl.ds(PAD + start - 1, size)] + acc[1, row, pl.ds(PAD + start, size)]
        total = total + acc[2, row, pl.ds(PAD + start + 1, size)]
        return jnp.maximum(total, 0.0)

    def outer(layer, chunk):
        start, size = span(layer, chunk)
        for side in range(2):
            place = 0 if side == 0 else rows + 1

            @pl.when(has_row[side])
            def _():
                for tile in range(2):
                    row_copy(layer, 1 - side, tile, chunk).wait_recv()
                for tile in range(2):
                    put(place, start, size, tile, halo[layer, side, tile, pl.ds(start, size)])

        def across(tap, carry):
            for place, row, down in ((0, 0, 0), (rows + 1, last, 2)):
                extra = jnp.dot(
                    sx[place, pl.ds(start, size)],
                    w3[layer, tap, pl.ds(down * 3 * chans, 3 * chans)],
                    preferred_element_type=jnp.float32,
                )
                acc[tap, row, pl.ds(PAD + start, size)] += extra
            return carry

        lax.fori_loop(0, 3, across, 0)

    chunks = len(cuts[0]) - 1
    load_x.wait()
    send_rows(0, 1, 0)
    for chunk in range(chunks):
        send_frames(0, chunk)
    split_weights(0)
    acc[:, :, pl.ds(0, PAD)] = jnp.zeros((3, rows, PAD, chans), jnp.float32)
    acc[:, :, pl.ds(PAD + cols, PAD)] = jnp.zeros((3, rows, PAD, chans), jnp.float32)
    for chunk in range(chunks):
        if chunk > 0:
            send_rows(0, 1, chunk)
        take_frames(0, chunk)
        lower_edges(0, chunk)
    for layer in range(layers):
        final = layer == layers - 1
        fill(layer)
        inner(layer)
        target = out if final else mid.at[layer]
        for row in range(1, last):
            target[row] = finish(row, 0, cols)
        for chunk in range(chunks):
            outer(layer, chunk)
            start = cuts[layer + 1][chunk]
            size = cuts[layer + 1][chunk + 1] - start
            for row in (0, last):
                target[row, pl.ds(start, size)] = finish(row, start, size)
            if not final:
                send_rows(layer + 1, 1, chunk)
                send_frames(layer + 1, chunk)
                if chunk == 0:
                    split_weights(layer + 1)
                take_frames(layer + 1, chunk)
                lower_edges(layer + 1, chunk)

    for layer in range(layers):
        for chunk in range(chunks):
            for side in range(2):

                @pl.when(has_row[side])
                def _():
                    for tile in range(2):
                        row_copy(layer, side, tile, chunk).wait_send()

                @pl.when(has_frame[side])
                def _():
                    frame_copy(layer, side, chunk).wait_send()


def store(y_ref, o_hbm, sem):
    copies = [pltpu.make_async_copy(y_ref.at[n], o_hbm.at[0, n], sem.at[n]) for n in range(y_ref.shape[0])]
    for copy in copies:
        copy.start()
    for copy in copies:
        copy.wait()


def local(features, conv_weight):
    _, rows, cols, chans = features.shape
    layers = conv_weight.shape[0]
    half, step = cols // 2, 2 * PAD
    cuts = [[0, half + step * (layers - 1 - n), cols] for n in range(layers)] + [[0, half - step, cols]]
    chunks = len(cuts[0]) - 1
    f32, bf16 = jnp.float32, jnp.bfloat16
    dma = pltpu.SemaphoreType.DMA
    result = pl.pallas_call(
        functools.partial(kernel, cuts),
        out_shape=pltpu.VMEM((rows, cols, chans), f32),
        in_specs=[pl.BlockSpec(memory_space=pl.ANY)] * 2,
        out_specs=pl.BlockSpec(memory_space=pltpu.VMEM),
        scratch_shapes=[
            pltpu.VMEM((rows, cols, chans), f32),
            pltpu.VMEM(conv_weight.shape, f32),
            pltpu.VMEM((layers, 3, 9 * chans, chans), bf16),
            pltpu.VMEM((rows + 2, cols, 3 * chans), bf16),
            pltpu.VMEM((3, rows, cols + 2 * PAD, chans), f32),
            pltpu.VMEM((layers - 1, rows, cols, chans), f32),
            pltpu.VMEM((layers, 2, 2, cols, LANES), f32),
            pltpu.VMEM((layers, 2, cols, LANES), f32),
            pltpu.VMEM((layers, 2, cols, LANES), f32),
            pltpu.VMEM((layers, 2, cols, LANES), f32),
            dma((layers + 1,)),
            dma((layers, 2, 2, chunks)),
            dma((layers, 2, 2, chunks)),
            dma((layers, 2, chunks)),
            dma((layers, 2, chunks)),
        ],
        compiler_params=pltpu.CompilerParams(
            collective_id=0, has_side_effects=True, vmem_limit_bytes=62 * 1024 * 1024
        ),
    )(features, conv_weight)
    return pl.pallas_call(
        store,
        out_shape=jax.ShapeDtypeStruct(features.shape, f32),
        in_specs=[pl.BlockSpec(memory_space=pltpu.VMEM)],
        out_specs=pl.BlockSpec(memory_space=pl.ANY),
        scratch_shapes=[dma((rows,))],
        compiler_params=pltpu.CompilerParams(vmem_limit_bytes=2 * 1024 * 1024),
    )(result)


def solution(mesh):
    placed = (P("frame", "row", None, None), P())
    return jax.shard_map(
        local, mesh=mesh, in_specs=placed, out_specs=P("frame", "row", None, None), check_vma=False
    )
```
